32 devices in a mesh: py: 4 (over y, x), px: 4 (over z), pz: 2 (over core).
Axes of the slice: x: 2, y: 2, z: 4, core: 2. Of those that a mesh axis runs over, the one named last changes fastest.
Arguments:
- tracer: float32 [32, 384, 16, 128], P('py', 'px', 'pz'), may hold values from 0.2 to 1.8
- flow_y: float32 [32, 384, 16, 128], P('py', 'px', 'pz'), may hold values from -0.3 to 0.3
- flow_x: float32 [32, 384, 16, 128], P('py', 'px', 'pz'), may hold values from -0.3 to 0.3
- flow_z: float32 [32, 384, 16, 128], P('py', 'px', 'pz'), may hold values from -0.3 to 0.3
Outputs:
- potential: float32 [32, 384, 16, 128], P('py', 'px', 'pz')
- tracer_end: float32 [32, 384, 16, 128], P('py', 'px', 'pz')
The draws below stay inside these ranges and needn't reach their ends.
All inputs are finite; a program needn't handle non-finite values.
Results may differ from the reference program's by a relative error of at most 0.00002.
Values sent between devices are 32-bit elements; how exact they have to be, the bound alone decides.
A program may use at most 128 MiB of HBM per device.

```python
import jax
import jax.numpy as jnp
from jax import lax

GRID_Y = 32
GRID_X = 384
GRID_Z = 16
MEMBERS = 128
STEPS = 4


def shard_levels(stream_key, shape, cuts, smallest, largest):
    def one(dim, parts):
        steps = jax.random.uniform(jax.random.fold_in(jax.random.fold_in(stream_key, 6), dim), (parts,), jnp.float32, smallest / len(cuts), largest / len(cuts))
        return jnp.repeat(jnp.exp(steps), shape[dim] // parts).reshape((-1,) + (1,) * (len(shape) - dim - 1))

    gain = one(*cuts[0])
    for cut in cuts[1:]:
        gain = gain * one(*cut)
    return gain


def setup_inputs(seed: int = 0) -> dict:
    streams_of = jax.random.split(jax.random.key(seed), 5)
    return {
        "tracer": jnp.clip(0.2 + 1.5999999 * jax.random.uniform(streams_of[0], (GRID_Y, GRID_X, GRID_Z, MEMBERS), jnp.float32) ** shard_levels(streams_of[0], (GRID_Y, GRID_X, GRID_Z, MEMBERS), ((0, 4), (1, 4), (2, 2)), -0.2, 0.2), 0.2, 1.8),
        "flow_y": jnp.clip(jax.random.uniform(streams_of[1], (GRID_Y, GRID_X, GRID_Z, MEMBERS), jnp.float32, -0.3, 0.3) * shard_levels(streams_of[1], (GRID_Y, GRID_X, GRID_Z, MEMBERS), ((0, 4), (1, 4), (2, 2)), -0.4, 0.0), -0.3, 0.3),
        "flow_x": jnp.clip(jax.random.uniform(streams_of[2], (GRID_Y, GRID_X, GRID_Z, MEMBERS), jnp.float32, -0.3, 0.3) * shard_levels(streams_of[2], (GRID_Y, GRID_X, GRID_Z, MEMBERS), ((0, 4), (1, 4), (2, 2)), -0.4, 0.0), -0.3, 0.3),
        "flow_z": jnp.clip(jax.random.uniform(streams_of[3], (GRID_Y, GRID_X, GRID_Z, MEMBERS), jnp.float32, -0.3, 0.3) * shard_levels(streams_of[3], (GRID_Y, GRID_X, GRID_Z, MEMBERS), ((0, 4), (1, 4), (2, 2)), -0.4, 0.0), -0.3, 0.3),
    }


def strip_edges(values, dims):
    for dim in dims:
        values = lax.slice_in_dim(values, 1, values.shape[dim] - 1, axis=dim)
    return values


def neighbour(values, dim, start, dims):
    others = [other for other in dims if other != dim]
    values = strip_edges(values, others)
    return lax.slice_in_dim(values, start, start + values.shape[dim] - 2, axis=dim)


def one_step(padded, flow_y, flow_x, flow_z):
    middle = strip_edges(padded, (0, 1, 2))
    lower = [neighbour(padded, dim, 0, (0, 1, 2)) for dim in (0, 1, 2)]
    upper = [neighbour(padded, dim, 2, (0, 1, 2)) for dim in (0, 1, 2)]
    slopes = [above - below for above, below in zip(upper, lower)]
    smooth_rate = 0.05
    spread = lower[0] + upper[0] + lower[1] + upper[1] + lower[2] + upper[2] - 6.0 * middle
    return middle - flow_y * slopes[0] - flow_x * slopes[1] - flow_z * slopes[2] + smooth_rate * spread


def reference(tracer, flow_y, flow_x, flow_z):
    for step in range(STEPS):
        tracer = one_step(jnp.pad(tracer, ((1, 1), (1, 1), (1, 1), (0, 0)), mode="constant"), flow_y, flow_x, flow_z)
    potential = jnp.cumsum(tracer, axis=2) / GRID_Z
    return potential, tracer
```

```python
import functools

import jax
import jax.numpy as jnp
from jax import lax
from jax.experimental import pallas as pl
from jax.experimental.pallas import tpu as pltpu
from jax.sharding import PartitionSpec as P

STEPS = 4
MESH = pl.DeviceIdType.MESH


def divisor(size, most):
    return max(d for d in range(1, most + 1) if size % d == 0)


class Axis:
    def __init__(self, name, count):
        self.name = name
        self.me = lax.axis_index(name)
        self.to = (self.me - 1, self.me + 1)
        self.sends = (self.me > 0, self.me < count - 1)
        self.gets = (self.sends[1], self.sends[0])


def kernel(counts, chunk, sub, tr, fy, fx, fz, pot, end, T, E, S, F, Z, load, ys, yr, xs, xr, zs, zr, zbs, zbr, eo, po, ebo, pbo):
    rows, width, depth, lanes = tr.shape
    chunks = width // chunk
    ay, ax, az = (Axis(n, c) for n, c in zip(("py", "px", "pz"), counts))
    flows = (fy, fx, fz)
    inner = rows - 2

    loads = [pltpu.make_async_copy(tr, T.at[0, pl.ds(1, rows), pl.ds(1, width)], load.at[0])]
    loads += [pltpu.make_async_copy(f, F.at[i], load.at[1 + i]) for i, f in enumerate(flows)]
    for copy in loads:
        copy.start()

    barrier = pltpu.get_barrier_semaphore()
    expect = 0
    for axis in (ay, ax, az):
        for d in (0, 1):
            @pl.when(axis.sends[d])
            def _():
                pl.semaphore_signal(barrier, inc=1, device_id={axis.name: axis.to[d]}, device_id_type=MESH)
            expect = expect + axis.sends[d].astype(jnp.int32)

    def blank(t):
        for d in (0, 1):
            @pl.when(jnp.logical_not(ay.gets[d]))
            def _():
                @pl.loop(0, chunks)
                def _(c):
                    T[t, rows + 1 if d == 0 else 0, pl.ds(1 + c * chunk, chunk)] = jnp.zeros((chunk, depth, lanes), jnp.float32)

            @pl.when(jnp.logical_not(ax.gets[d]))
            def _():
                T[t, pl.ds(1, rows), pl.ds(width + 1 if d == 0 else 0, 1)] = jnp.zeros((rows, 1, depth, lanes), jnp.float32)

    for t in range(STEPS):
        blank(t)
    pl.semaphore_wait(barrier, expect)

    def remote(src, dst, ssem, rsem, axis, d):
        return pltpu.make_async_remote_copy(
            src_ref=src, dst_ref=dst, send_sem=ssem, recv_sem=rsem,
            device_id={axis.name: axis.to[d]}, device_id_type=MESH,
        )

    def ycopy(t, d, c):
        at = c * chunk
        if t == 0:
            src = tr.at[0 if d == 0 else rows - 1, pl.ds(at, chunk)]
        else:
            src = T.at[t, 1 if d == 0 else rows, pl.ds(1 + at, chunk)]
        dst = T.at[t, rows + 1 if d == 0 else 0, pl.ds(1 + at, chunk)]
        return remote(src, dst, ys.at[t, d, c], yr.at[t, d, c], ay, d)

    def xcopy(t, d):
        if t == 0:
            src = tr.at[:, pl.ds(0 if d == 0 else width - 1, 1)]
        else:
            src = T.at[t, pl.ds(1, rows), pl.ds(1 if d == 0 else width, 1)]
        dst = T.at[t, pl.ds(1, rows), pl.ds(width + 1 if d == 0 else 0, 1)]
        return remote(src, dst, xs.at[t, d], xr.at[t, d], ax, d)

    def zrefs(t, d, y, ny, x, nx):
        row = pl.ds(0 if d == 0 else depth - 1, 1)
        if t < STEPS:
            src = T.at[t, pl.ds(1 + y, ny), pl.ds(1 + x, nx), row]
        else:
            src = S.at[pl.ds(y, ny), pl.ds(x, nx), row]
        return src, Z.at[t, pl.ds(y, ny), pl.ds(x, nx), row]

    def zcopy(t, d):
        return remote(*zrefs(t, d, 1, inner, 0, width), zs.at[t, d], zr.at[t, d], az, d)

    def zbcopy(t, d, c, b):
        return remote(
            *zrefs(t, d, 0 if b == 0 else rows - 1, 1, c * chunk, chunk),
            zbs.at[t, d, c, b], zbr.at[t, d, c, b], az, d,
        )

    def start(flag, copy):
        @pl.when(flag)
        def _():
            copy.start()

    def arrived(flag, copy):
        @pl.when(flag)
        def _():
            copy.wait_recv()

    level = lax.broadcasted_iota(jnp.int32, (sub, depth, lanes), 1)
    known = (level == jnp.where(az.gets[0], 0, -1)) | (level == jnp.where(az.gets[1], depth - 1, -1))
    first, last = level == 0, level == depth - 1
    share = 1.0 / (depth * counts[2])

    def cells(t, y, x):
        line = T[t, 1 + y, pl.ds(x, sub + 2)]
        here, x_low, x_high = line[1:-1], line[:-2], line[2:]
        y_low = T[t, y, pl.ds(1 + x, sub)]
        y_high = T[t, y + 2, pl.ds(1 + x, sub)]
        beside = jnp.where(known, Z[t, y, pl.ds(x, sub)], 0.0)
        z_low = pltpu.roll(jnp.where(last, beside, here), 1, 1)
        z_high = pltpu.roll(jnp.where(first, beside, here), depth - 1, 1)
        spread = y_low + y_high + x_low + x_high + z_low + z_high - 6.0 * here
        new = (
            here - F[0, y, pl.ds(x, sub)] * (y_high - y_low) - F[1, y, pl.ds(x, sub)] * (x_high - x_low)
            - F[2, y, pl.ds(x, sub)] * (z_high - z_low) + 0.05 * spread
        )
        if t < STEPS - 1:
            T[t + 1, 1 + y, pl.ds(1 + x, sub)] = new
        else:
            E[y, pl.ds(x, sub)] = new
            total, reach = new, 1
            while reach < depth:
                total = total + jnp.where(level >= reach, pltpu.roll(total, reach, 1), 0.0)
                reach *= 2
            S[y, pl.ds(x, sub)] = total * share

    def add_below(y, x):
        low = Z[STEPS, y, pl.ds(x, sub), pl.ds(depth - 1, 1)]
        S[y, pl.ds(x, sub)] = S[y, pl.ds(x, sub)] + low

    def out(ref, to, y, ny, x, nx, sem):
        return pltpu.make_async_copy(
            ref.at[pl.ds(y, ny), pl.ds(x, nx)], to.at[pl.ds(y, ny), pl.ds(x, nx)], sem
        )

    def ends(c, b):
        return out(E, end, 0 if b == 0 else rows - 1, 1, c * chunk, chunk, ebo.at[c, b])

    def pots(c, b):
        return out(S, pot, 0 if b == 0 else rows - 1, 1, c * chunk, chunk, pbo.at[c, b])

    end_inner = out(E, end, 1, inner, 0, width, eo)
    pot_inner = out(S, pot, 1, inner, 0, width, po)

    @pl.loop(0, chunks)
    def _(c):
        for d in (0, 1):
            start(ay.sends[d], ycopy(0, d, c))
    for d in (0, 1):
        start(ax.sends[d], xcopy(0, d))
    loads[0].wait()
    for d in (0, 1):
        start(az.sends[d], zcopy(0, d))

        @pl.loop(0, chunks)
        def _(c):
            for b in (0, 1):
                start(az.sends[d], zbcopy(0, d, c, b))
    for copy in loads[1:]:
        copy.wait()

    subs = width // sub
    for t in range(STEPS):
        for d in (0, 1):
            arrived(ax.gets[d], xcopy(t, d))
            arrived(az.gets[d], zcopy(t, d))

        @pl.loop(0, inner * subs)
        def _(i):
            cells(t, 1 + i // subs, (i % subs) * sub)

        if t < STEPS - 1:
            for d in (0, 1):
                start(az.sends[d], zcopy(t + 1, d))
        else:
            end_inner.start()

            @pl.when(az.gets[1])
            def _():
                zcopy(STEPS, 1).wait_recv()

                @pl.loop(0, inner * subs)
                def _(i):
                    add_below(1 + i // subs, (i % subs) * sub)
            start(az.sends[1], zcopy(STEPS, 1))
            pot_inner.start()

        @pl.loop(0, chunks)
        def _(c):
            for d in (0, 1):
                arrived(ay.gets[d], ycopy(t, d, c))
                for b in (0, 1):
                    arrived(az.gets[d], zbcopy(t, d, c, b))
            for b, y in ((0, 0), (1, rows - 1)):
                @pl.loop(0, chunk // sub)
                def _(i):
                    cells(t, y, c * chunk + i * sub)
                if t < STEPS - 1:
                    start(ay.sends[b], ycopy(t + 1, b, c))
                    for d in (0, 1):
                        start(az.sends[d], zbcopy(t + 1, d, c, b))
                else:
                    ends(c, b).start()

        if t < STEPS - 1:
            for d in (0, 1):
                start(ax.sends[d], xcopy(t + 1, d))

    @pl.loop(0, chunks)
    def _(c):
        for b, y in ((0, 0), (1, rows - 1)):
            @pl.when(az.gets[1])
            def _():
                zbcopy(STEPS, 1, c, b).wait_recv()

                @pl.loop(0, chunk // sub)
                def _(i):
                    add_below(y, c * chunk + i * sub)
            start(az.sends[1], zbcopy(STEPS, 1, c, b))
            pots(c, b).start()

    def left(flag, copy):
        @pl.when(flag)
        def _():
            copy.wait_send()

    for t in range(STEPS + 1):
        for d in (0, 1):
            if t < STEPS:
                left(ax.sends[d], xcopy(t, d))
            if t < STEPS or d == 1:
                left(az.sends[d], zcopy(t, d))

        @pl.loop(0, chunks)
        def _(c):
            for d in (0, 1):
                if t < STEPS:
                    left(ay.sends[d], ycopy(t, d, c))
                if t < STEPS or d == 1:
                    for b in (0, 1):
                        left(az.sends[d], zbcopy(t, d, c, b))
    end_inner.wait()
    pot_inner.wait()

    @pl.loop(0, chunks)
    def _(c):
        for b in (0, 1):
            ends(c, b).wait()
            pots(c, b).wait()


def local(counts, tracer, flow_y, flow_x, flow_z):
    rows, width, depth, lanes = tracer.shape
    chunk = divisor(width, 16)
    sub = divisor(chunk, 8)
    chunks = width // chunk
    block = jax.ShapeDtypeStruct(tracer.shape, jnp.float32)
    dma = pltpu.SemaphoreType.DMA
    return pl.pallas_call(
        functools.partial(kernel, counts, chunk, sub),
        out_shape=(block, block),
        in_specs=[pl.BlockSpec(memory_space=pl.ANY)] * 4,
        out_specs=[pl.BlockSpec(memory_space=pl.ANY)] * 2,
        scratch_shapes=[
            pltpu.VMEM((STEPS, rows + 2, width + 2, depth, lanes), jnp.float32),
            pltpu.VMEM(tracer.shape, jnp.float32),
            pltpu.VMEM(tracer.shape, jnp.float32),
            pltpu.VMEM((3,) + tracer.shape, jnp.float32),
            pltpu.VMEM((STEPS + 1,) + tracer.shape, jnp.float32),
            dma((4,)),
            dma((STEPS, 2, chunks)),
            dma((STEPS, 2, chunks)),
            dma((STEPS, 2)),
            dma((STEPS, 2)),
            dma((STEPS + 1, 2)),
            dma((STEPS + 1, 2)),
            dma((STEPS + 1, 2, chunks, 2)),
            dma((STEPS + 1, 2, chunks, 2)),
            dma(()),
            dma(()),
            dma((chunks, 2)),
            dma((chunks, 2)),
        ],
        compiler_params=pltpu.CompilerParams(
            collective_id=0, has_side_effects=True, vmem_limit_bytes=60 * 1024 * 1024
        ),
    )(tracer, flow_y, flow_x, flow_z)


def solution(mesh):
    counts = tuple(mesh.shape[name] for name in ("py", "px", "pz"))
    placed = P("py", "px", "pz", None)
    return jax.shard_map(
        functools.partial(local, counts),
        mesh=mesh,
        in_specs=(placed,) * 4,
        out_specs=(placed, placed),
        check_vma=False,
    )
```

```python
import functools

import jax
import jax.numpy as jnp
from jax import lax
from jax.experimental import pallas as pl
from jax.experimental.pallas import tpu as pltpu
from jax.sharding import PartitionSpec as P

STEPS = 4
MESH = pl.DeviceIdType.MESH


def divisor(size, most):
    return max(d for d in range(1, most + 1) if size % d == 0)


class Axis:
    def __init__(self, name, count):
        self.name = name
        self.me = lax.axis_index(name)
        self.to = (self.me - 1, self.me + 1)
        self.sends = (self.me > 0, self.me < count - 1)
        self.gets = (self.sends[1], self.sends[0])


def kernel(counts, relays, chunk, sub, tr, fy, fx, fz, S, E, T, F, Z, R, load, rs, rr, ys, yr, xs, xr, zs, zr, zbs, zbr):
    rows, width, depth, lanes = tr.shape
    chunks = width // chunk
    ay, ax, az = (Axis(n, c) for n, c in zip(("py", "px", "pz"), counts))
    flows = (fy, fx, fz)
    inner = rows - 2
    direct = chunks // 2

    loads = [pltpu.make_async_copy(tr, T.at[0, pl.ds(1, rows), pl.ds(1, width)], load.at[0])]
    loads += [pltpu.make_async_copy(f, F.at[i], load.at[1 + i]) for i, f in enumerate(flows)]
    for copy in loads:
        copy.start()

    barrier = pltpu.get_barrier_semaphore()
    expect = 0
    for axis in (ay, ax, az):
        for d in (0, 1):
            @pl.when(axis.sends[d])
            def _():
                pl.semaphore_signal(barrier, inc=1, device_id={axis.name: axis.to[d]}, device_id_type=MESH)
            expect = expect + axis.sends[d].astype(jnp.int32)
    pairs = {frozenset((a, r)) for a, d, r in relays} | {frozenset((r, a + 2 * d - 1)) for a, d, r in relays}
    for one, other in sorted(sorted(p) for p in pairs):
        if other - one == 1:
            continue
        for a, b in ((one, other), (other, one)):
            @pl.when(ay.me == a)
            def _():
                pl.semaphore_signal(barrier, inc=1, device_id={"py": b}, device_id_type=MESH)
            expect = expect + (ay.me == a).astype(jnp.int32)

    def blank(t):
        for d in (0, 1):
            @pl.when(jnp.logical_not(ay.gets[d]))
            def _():
                @pl.loop(0, chunks)
                def _(c):
                    T[t, rows + 1 if d == 0 else 0, pl.ds(1 + c * chunk, chunk)] = jnp.zeros((chunk, depth, lanes), jnp.float32)

            @pl.when(jnp.logical_not(ax.gets[d]))
            def _():
                T[t, pl.ds(1, rows), pl.ds(width + 1 if d == 0 else 0, 1)] = jnp.zeros((rows, 1, depth, lanes), jnp.float32)

    for t in range(STEPS):
        blank(t)
    pl.semaphore_wait(barrier, expect)

    def remote(src, dst, ssem, rsem, axis, d, to=None):
        return pltpu.make_async_remote_copy(
            src_ref=src, dst_ref=dst, send_sem=ssem, recv_sem=rsem,
            device_id={axis.name: axis.to[d] if to is None else to}, device_id_type=MESH,
        )

    def ycopy(t, d, c, relay=None):
        at = c * chunk
        if t == 0:
            src = tr.at[0 if d == 0 else rows - 1, pl.ds(at, chunk)]
        else:
            src = T.at[t, 1 if d == 0 else rows, pl.ds(1 + at, chunk)]
        if relay is not None:
            return remote(src, R.at[t, pl.ds(at, chunk)], ys.at[t, d, c], rr.at[t, c], ay, d, relay)
        dst = T.at[t, rows + 1 if d == 0 else 0, pl.ds(1 + at, chunk)]
        return remote(src, dst, ys.at[t, d, c], yr.at[t, d, c], ay, d)

    def ysend(t, d, c):
        plain = ay.sends[d]
        for a, way, relay in relays:
            if way == d:
                turn = (ay.me == a) & (c >= direct)
                plain = plain & jnp.logical_not(turn)
                start(turn, ycopy(t, d, c, relay))
        start(plain, ycopy(t, d, c))

    def passed(t, a, d, c):
        at = c * chunk
        dst = T.at[t, rows + 1 if d == 0 else 0, pl.ds(1 + at, chunk)]
        return remote(R.at[t, pl.ds(at, chunk)], dst, rs.at[t, c], yr.at[t, d, c], ay, d, a + 2 * d - 1)

    def pass_on(t):
        for a, d, relay in relays:
            @pl.when(ay.me == relay)
            def _():
                @pl.loop(direct, chunks)
                def _(c):
                    ycopy(t, d, c, relay).wait_recv()
                    passed(t, a, d, c).start()

    def xcopy(t, d):
        if t == 0:
            src = tr.at[:, pl.ds(0 if d == 0 else width - 1, 1)]
        else:
            src = T.at[t, pl.ds(1, rows), pl.ds(1 if d == 0 else width, 1)]
        dst = T.at[t, pl.ds(1, rows), pl.ds(width + 1 if d == 0 else 0, 1)]
        return remote(src, dst, xs.at[t, d], xr.at[t, d], ax, d)

    def zrefs(t, d, y, ny, x, nx):
        row = pl.ds(0 if d == 0 else depth - 1, 1)
        if t < STEPS:
            src = T.at[t, pl.ds(1 + y, ny), pl.ds(1 + x, nx), row]
        else:
            src = S.at[pl.ds(y, ny), pl.ds(x, nx), row]
        return src, Z.at[t, pl.ds(y, ny), pl.ds(x, nx), row]

    def zcopy(t, d):
        return remote(*zrefs(t, d, 1, inner, 0, width), zs.at[t, d], zr.at[t, d], az, d)

    def zbcopy(t, d, c, b):
        return remote(
            *zrefs(t, d, 0 if b == 0 else rows - 1, 1, c * chunk, chunk),
            zbs.at[t, d, c, b], zbr.at[t, d, c, b], az, d,
        )

    def start(flag, copy):
        @pl.when(flag)
        def _():
            copy.start()

    def arrived(flag, copy):
        @pl.when(flag)
        def _():
            copy.wait_recv()

    level = lax.broadcasted_iota(jnp.int32, (sub, depth, lanes), 1)
    known = (level == jnp.where(az.gets[0], 0, -1)) | (level == jnp.where(az.gets[1], depth - 1, -1))
    first, last = level == 0, level == depth - 1
    share = 1.0 / (depth * counts[2])

    def cells(t, y, x):
        line = T[t, 1 + y, pl.ds(x, sub + 2)]
        here, x_low, x_high = line[1:-1], line[:-2], line[2:]
        y_low = T[t, y, pl.ds(1 + x, sub)]
        y_high = T[t, y + 2, pl.ds(1 + x, sub)]
        beside = jnp.where(known, Z[t, y, pl.ds(x, sub)], 0.0)
        z_low = pltpu.roll(jnp.where(last, beside, here), 1, 1)
        z_high = pltpu.roll(jnp.where(first, beside, here), depth - 1, 1)
        spread = y_low + y_high + x_low + x_high + z_low + z_high - 6.0 * here
        new = (
            here - F[0, y, pl.ds(x, sub)] * (y_high - y_low) - F[1, y, pl.ds(x, sub)] * (x_high - x_low)
            - F[2, y, pl.ds(x, sub)] * (z_high - z_low) + 0.05 * spread
        )
        if t < STEPS - 1:
            T[t + 1, 1 + y, pl.ds(1 + x, sub)] = new
        else:
            E[y, pl.ds(x, sub)] = new
            total, reach = new, 1
            while reach < depth:
                total = total + jnp.where(level >= reach, pltpu.roll(total, reach, 1), 0.0)
                reach *= 2
            S[y, pl.ds(x, sub)] = total * share

    def add_below(y, x):
        low = Z[STEPS, y, pl.ds(x, sub), pl.ds(depth - 1, 1)]
        S[y, pl.ds(x, sub)] = S[y, pl.ds(x, sub)] + low

    @pl.loop(0, chunks)
    def _(c):
        for d in (0, 1):
            ysend(0, d, c)
    for d in (0, 1):
        start(ax.sends[d], xcopy(0, d))
    loads[0].wait()
    for d in (0, 1):
        start(az.sends[d], zcopy(0, d))

        @pl.loop(0, chunks)
        def _(c):
            for b in (0, 1):
                start(az.sends[d], zbcopy(0, d, c, b))
    pass_on(0)
    for copy in loads[1:]:
        copy.wait()

    subs = width // sub
    for t in range(STEPS):
        for d in (0, 1):
            arrived(ax.gets[d], xcopy(t, d))
            arrived(az.gets[d], zcopy(t, d))

        @pl.loop(0, inner * subs)
        def _(i):
            cells(t, 1 + i // subs, (i % subs) * sub)

        if t < STEPS - 1:
            for d in (0, 1):
                start(az.sends[d], zcopy(t + 1, d))
        else:
            @pl.when(az.gets[1])
            def _():
                zcopy(STEPS, 1).wait_recv()

                @pl.loop(0, inner * subs)
                def _(i):
                    add_below(1 + i // subs, (i % subs) * sub)
            start(az.sends[1], zcopy(STEPS, 1))
        if t > 0:
            pass_on(t)

        @pl.loop(0, chunks)
        def _(c):
            for d in (0, 1):
                arrived(ay.gets[d], ycopy(t, d, c))
                for b in (0, 1):
                    arrived(az.gets[d], zbcopy(t, d, c, b))
            for b, y in ((0, 0), (1, rows - 1)):
                @pl.loop(0, chunk // sub)
                def _(i):
                    cells(t, y, c * chunk + i * sub)
                if t < STEPS - 1:
                    ysend(t + 1, b, c)
                    for d in (0, 1):
                        start(az.sends[d], zbcopy(t + 1, d, c, b))

        if t < STEPS - 1:
            for d in (0, 1):
                start(ax.sends[d], xcopy(t + 1, d))

    @pl.loop(0, chunks)
    def _(c):
        for b, y in ((0, 0), (1, rows - 1)):
            @pl.when(az.gets[1])
            def _():
                zbcopy(STEPS, 1, c, b).wait_recv()

                @pl.loop(0, chunk // sub)
                def _(i):
                    add_below(y, c * chunk + i * sub)
            start(az.sends[1], zbcopy(STEPS, 1, c, b))

    def left(flag, copy):
        @pl.when(flag)
        def _():
            copy.wait_send()

    for a, d, relay in relays:
        @pl.when(ay.me == relay)
        def _():
            for t in range(STEPS):
                @pl.loop(direct, chunks)
                def _(c):
                    passed(t, a, d, c).wait_send()

    for t in range(STEPS + 1):
        for d in (0, 1):
            if t < STEPS:
                left(ax.sends[d], xcopy(t, d))
            if t < STEPS or d == 1:
                left(az.sends[d], zcopy(t, d))

        @pl.loop(0, chunks)
        def _(c):
            for d in (0, 1):
                if t < STEPS:
                    left(ay.sends[d], ycopy(t, d, c))
                if t < STEPS or d == 1:
                    for b in (0, 1):
                        left(az.sends[d], zbcopy(t, d, c, b))


def local(counts, relays, tracer, flow_y, flow_x, flow_z):
    rows, width, depth, lanes = tracer.shape
    chunk = divisor(width, 16)
    sub = divisor(chunk, 8)
    chunks = width // chunk
    block = pltpu.VMEM(tracer.shape, jnp.float32)
    dma = pltpu.SemaphoreType.DMA
    return pl.pallas_call(
        functools.partial(kernel, counts, relays, chunk, sub),
        out_shape=(block, block),
        in_specs=[pl.BlockSpec(memory_space=pl.ANY)] * 4,
        out_specs=[pl.BlockSpec(memory_space=pltpu.VMEM)] * 2,
        scratch_shapes=[
            pltpu.VMEM((STEPS, rows + 2, width + 2, depth, lanes), jnp.float32),
            pltpu.VMEM((3,) + tracer.shape, jnp.float32),
            pltpu.VMEM((STEPS + 1,) + tracer.shape, jnp.float32),
            pltpu.VMEM((STEPS, width, depth, lanes), jnp.float32),
            dma((4,)),
            dma((STEPS, chunks)),
            dma((STEPS, chunks)),
            dma((STEPS, 2, chunks)),
            dma((STEPS, 2, chunks)),
            dma((STEPS, 2)),
            dma((STEPS, 2)),
            dma((STEPS + 1, 2)),
            dma((STEPS + 1, 2)),
            dma((STEPS + 1, 2, chunks, 2)),
            dma((STEPS + 1, 2, chunks, 2)),
        ],
        compiler_params=pltpu.CompilerParams(
            collective_id=0, has_side_effects=True, vmem_limit_bytes=50 * 1024 * 1024
        ),
    )(tracer, flow_y, flow_x, flow_z)


KEEP = 0


def detours(mesh):
    spots = [getattr(device, "coords", None) for device in mesh.devices[:, 0, 0]]
    if any(spot is None for spot in spots):
        return ()
    gap = lambda a, b: [i for i, (p, q) in enumerate(zip(spots[a], spots[b])) if p != q]
    found, busy = [], set()
    for a in range(len(spots)):
        for d, b in ((0, a - 1), (1, a + 1)):
            if not 0 <= b < len(spots) or len(gap(a, b)) != 2:
                continue
            kept, other = gap(a, b)[KEEP], gap(a, b)[1 - KEEP]
            for r in range(len(spots)):
                if r not in busy and gap(a, r) == [other] and gap(r, b) == [kept]:
                    busy.add(r)
                    found.append((a, d, r))
                    break
    return tuple(found)


def solution(mesh):
    counts = tuple(mesh.shape[name] for name in ("py", "px", "pz"))
    placed = P("py", "px", "pz", None)
    return jax.shard_map(
        functools.partial(local, counts, detours(mesh)),
        mesh=mesh,
        in_specs=(placed,) * 4,
        out_specs=(placed, placed),
        check_vma=False,
    )
```

```python
import functools

import jax
import jax.numpy as jnp
from jax import lax
from jax.experimental import pallas as pl
from jax.experimental.pallas import tpu as pltpu
from jax.sharding import PartitionSpec as P

STEPS = 4
MESH = pl.DeviceIdType.MESH


def divisor(size, most):
    return max(d for d in range(1, most + 1) if size % d == 0)


class Axis:
    def __init__(self, name, count):
        self.name = name
        self.me = lax.axis_index(name)
        self.to = (self.me - 1, self.me + 1)
        self.sends = (self.me > 0, self.me < count - 1)
        self.gets = (self.sends[1], self.sends[0])


def kernel(counts, relays, chunk, sub, tr, fy, fx, fz, S, E, T, F, Z, R, load, rs, rr, ys, yr, xs, xr, zs, zr, zbs, zbr):
    rows, width, depth, lanes = tr.shape
    chunks = width // chunk
    ay, ax, az = (Axis(n, c) for n, c in zip(("py", "px", "pz"), counts))
    flows = (fy, fx, fz)
    inner = rows - 2
    direct = chunks // 2

    loads = [
        pltpu.make_async_copy(tr.at[pl.ds(y, n)], T.at[0, pl.ds(1 + y, n), pl.ds(1, width)], load.at[i])
        for i, (y, n) in enumerate(((0, 1), (rows - 1, 1), (1, inner)))
    ]
    loads += [pltpu.make_async_copy(f, F.at[i], load.at[3 + i]) for i, f in enumerate(flows)]
    for copy in loads[:3]:
        copy.start()

    barrier = pltpu.get_barrier_semaphore()
    expect = 0
    for axis in (ay, ax, az):
        for d in (0, 1):
            @pl.when(axis.sends[d])
            def _():
                pl.semaphore_signal(barrier, inc=1, device_id={axis.name: axis.to[d]}, device_id_type=MESH)
            expect = expect + axis.sends[d].astype(jnp.int32)
    pairs = {frozenset((a, r)) for a, d, r in relays} | {frozenset((r, a + 2 * d - 1)) for a, d, r in relays}
    for one, other in sorted(sorted(p) for p in pairs):
        if other - one == 1:
            continue
        for a, b in ((one, other), (other, one)):
            @pl.when(ay.me == a)
            def _():
                pl.semaphore_signal(barrier, inc=1, device_id={"py": b}, device_id_type=MESH)
            expect = expect + (ay.me == a).astype(jnp.int32)

    def blank(t):
        for d in (0, 1):
            @pl.when(jnp.logical_not(ay.gets[d]))
            def _():
                @pl.loop(0, chunks)
                def _(c):
                    T[t, rows + 1 if d == 0 else 0, pl.ds(1 + c * chunk, chunk)] = jnp.zeros((chunk, depth, lanes), jnp.float32)

            @pl.when(jnp.logical_not(ax.gets[d]))
            def _():
                T[t, pl.ds(1, rows), pl.ds(width + 1 if d == 0 else 0, 1)] = jnp.zeros((rows, 1, depth, lanes), jnp.float32)

    for t in range(STEPS):
        blank(t)
    pl.semaphore_wait(barrier, expect)

    def remote(src, dst, ssem, rsem, axis, d, to=None):
        return pltpu.make_async_remote_copy(
            src_ref=src, dst_ref=dst, send_sem=ssem, recv_sem=rsem,
            device_id={axis.name: axis.to[d] if to is None else to}, device_id_type=MESH,
        )

    def ycopy(t, d, c, relay=None):
        at = c * chunk
        src = T.at[t, 1 if d == 0 else rows, pl.ds(1 + at, chunk)]
        if relay is not None:
            return remote(src, R.at[t, pl.ds(at, chunk)], ys.at[t, d, c], rr.at[t, c], ay, d, relay)
        dst = T.at[t, rows + 1 if d == 0 else 0, pl.ds(1 + at, chunk)]
        return remote(src, dst, ys.at[t, d, c], yr.at[t, d, c], ay, d)

    def detoured(t):
        return (direct, chunks) if t == 0 else (0, direct)

    def ysend(t, d, c):
        plain = ay.sends[d]
        for a, way, relay in relays:
            if way == d:
                turn = (ay.me == a) & ((c >= direct) if t == 0 else (c < direct))
                plain = plain & jnp.logical_not(turn)
                start(turn, ycopy(t, d, c, relay))
        start(plain, ycopy(t, d, c))

    def passed(t, a, d, c):
        at = c * chunk
        dst = T.at[t, rows + 1 if d == 0 else 0, pl.ds(1 + at, chunk)]
        return remote(R.at[t, pl.ds(at, chunk)], dst, rs.at[t, c], yr.at[t, d, c], ay, d, a + 2 * d - 1)

    def pass_on(t):
        for a, d, relay in relays:
            @pl.when(ay.me == relay)
            def _():
                @pl.loop(*detoured(t))
                def _(c):
                    ycopy(t, d, c, relay).wait_recv()
                    passed(t, a, d, c).start()

    def xcopy(t, d):
        src = T.at[t, pl.ds(1, rows), pl.ds(1 if d == 0 else width, 1)]
        dst = T.at[t, pl.ds(1, rows), pl.ds(width + 1 if d == 0 else 0, 1)]
        return remote(src, dst, xs.at[t, d], xr.at[t, d], ax, d)

    def zrefs(t, d, y, ny, x, nx):
        row = pl.ds(0 if d == 0 else depth - 1, 1)
        if t < STEPS:
            src = T.at[t, pl.ds(1 + y, ny), pl.ds(1 + x, nx), row]
        else:
            src = S.at[pl.ds(y, ny), pl.ds(x, nx), row]
        return src, Z.at[t, pl.ds(y, ny), pl.ds(x, nx), row]

    def zcopy(t, d):
        return remote(*zrefs(t, d, 1, inner, 0, width), zs.at[t, d], zr.at[t, d], az, d)

    def zbcopy(t, d, c, b):
        return remote(
            *zrefs(t, d, 0 if b == 0 else rows - 1, 1, c * chunk, chunk),
            zbs.at[t, d, c, b], zbr.at[t, d, c, b], az, d,
        )

    def start(flag, copy):
        @pl.when(flag)
        def _():
            copy.start()

    def arrived(flag, copy):
        @pl.when(flag)
        def _():
            copy.wait_recv()

    level = lax.broadcasted_iota(jnp.int32, (sub, depth, lanes), 1)
    known = (level == jnp.where(az.gets[0], 0, -1)) | (level == jnp.where(az.gets[1], depth - 1, -1))
    first, last = level == 0, level == depth - 1
    share = 1.0 / (depth * counts[2])

    def cells(t, y, x):
        line = T[t, 1 + y, pl.ds(x, sub + 2)]
        here, x_low, x_high = line[1:-1], line[:-2], line[2:]
        y_low = T[t, y, pl.ds(1 + x, sub)]
        y_high = T[t, y + 2, pl.ds(1 + x, sub)]
        beside = jnp.where(known, Z[t, y, pl.ds(x, sub)], 0.0)
        z_low = pltpu.roll(jnp.where(last, beside, here), 1, 1)
        z_high = pltpu.roll(jnp.where(first, beside, here), depth - 1, 1)
        spread = y_low + y_high + x_low + x_high + z_low + z_high - 6.0 * here
        new = (
            here - F[0, y, pl.ds(x, sub)] * (y_high - y_low) - F[1, y, pl.ds(x, sub)] * (x_high - x_low)
            - F[2, y, pl.ds(x, sub)] * (z_high - z_low) + 0.05 * spread
        )
        if t < STEPS - 1:
            T[t + 1, 1 + y, pl.ds(1 + x, sub)] = new
        else:
            E[y, pl.ds(x, sub)] = new
            total, reach = new, 1
            while reach < depth:
                total = total + jnp.where(level >= reach, pltpu.roll(total, reach, 1), 0.0)
                reach *= 2
            S[y, pl.ds(x, sub)] = total * share

    def add_below(y, x):
        low = Z[STEPS, y, pl.ds(x, sub), pl.ds(depth - 1, 1)]
        S[y, pl.ds(x, sub)] = S[y, pl.ds(x, sub)] + low

    def finish(c):
        for b, y in ((0, 0), (1, rows - 1)):
            zbcopy(STEPS, 1, c, b).wait_recv()

            @pl.loop(0, chunk // sub)
            def _(i):
                add_below(y, c * chunk + i * sub)
            start(az.sends[1], zbcopy(STEPS, 1, c, b))

    loads[0].wait()
    loads[1].wait()

    @pl.loop(0, chunks)
    def _(c):
        for d in (0, 1):
            ysend(0, d, c)
    for copy in loads[3:]:
        copy.start()
    loads[2].wait()
    for d in (0, 1):
        start(ax.sends[d], xcopy(0, d))
    for d in (0, 1):
        start(az.sends[d], zcopy(0, d))

        @pl.loop(0, chunks)
        def _(c):
            for b in (0, 1):
                start(az.sends[d], zbcopy(0, d, c, b))
    pass_on(0)
    for copy in loads[3:]:
        copy.wait()

    subs = width // sub
    for t in range(STEPS):
        for d in (0, 1):
            arrived(ax.gets[d], xcopy(t, d))
            arrived(az.gets[d], zcopy(t, d))

        @pl.loop(0, inner * subs)
        def _(i):
            cells(t, 1 + i // subs, (i % subs) * sub)

        if t < STEPS - 1:
            for d in (0, 1):
                start(az.sends[d], zcopy(t + 1, d))
        else:
            @pl.when(az.gets[1])
            def _():
                zcopy(STEPS, 1).wait_recv()

                @pl.loop(0, inner * subs)
                def _(i):
                    add_below(1 + i // subs, (i % subs) * sub)
            start(az.sends[1], zcopy(STEPS, 1))
        @pl.loop(0, chunks)
        def _(c):
            if t < STEPS - 1:
                @pl.when(c == direct)
                def _():
                    pass_on(t + 1)
            for d in (0, 1):
                arrived(ay.gets[d], ycopy(t, d, c))
                for b in (0, 1):
                    arrived(az.gets[d], zbcopy(t, d, c, b))
            for b, y in ((0, 0), (1, rows - 1)):
                @pl.loop(0, chunk // sub)
                def _(i):
                    cells(t, y, c * chunk + i * sub)
                if t < STEPS - 1:
                    ysend(t + 1, b, c)
                    for d in (0, 1):
                        start(az.sends[d], zbcopy(t + 1, d, c, b))
                else:
                    start(az.sends[1] & jnp.logical_not(az.gets[1]), zbcopy(STEPS, 1, c, b))
            if t == STEPS - 1:
                @pl.when(az.gets[1] & (c > 0))
                def _():
                    finish(c - 1)

        if t < STEPS - 1:
            for d in (0, 1):
                start(ax.sends[d], xcopy(t + 1, d))

    @pl.when(az.gets[1])
    def _():
        finish(chunks - 1)

    def left(flag, copy):
        @pl.when(flag)
        def _():
            copy.wait_send()

    for a, d, relay in relays:
        @pl.when(ay.me == relay)
        def _():
            for t in range(STEPS):
                @pl.loop(*detoured(t))
                def _(c):
                    passed(t, a, d, c).wait_send()

    for t in range(STEPS + 1):
        for d in (0, 1):
            if t < STEPS:
                left(ax.sends[d], xcopy(t, d))
            if t < STEPS or d == 1:
                left(az.sends[d], zcopy(t, d))

        @pl.loop(0, chunks)
        def _(c):
            for d in (0, 1):
                if t < STEPS:
                    left(ay.sends[d], ycopy(t, d, c))
                if t < STEPS or d == 1:
                    for b in (0, 1):
                        left(az.sends[d], zbcopy(t, d, c, b))


def local(counts, relays, tracer, flow_y, flow_x, flow_z):
    rows, width, depth, lanes = tracer.shape
    chunk = divisor(width, 48)
    sub = divisor(chunk, 8)
    chunks = width // chunk
    block = pltpu.VMEM(tracer.shape, jnp.float32)
    dma = pltpu.SemaphoreType.DMA
    return pl.pallas_call(
        functools.partial(kernel, counts, relays, chunk, sub),
        out_shape=(block, block),
        in_specs=[pl.BlockSpec(memory_space=pl.ANY)] * 4,
        out_specs=[pl.BlockSpec(memory_space=pltpu.VMEM)] * 2,
        scratch_shapes=[
            pltpu.VMEM((STEPS, rows + 2, width + 2, depth, lanes), jnp.float32),
            pltpu.VMEM((3,) + tracer.shape, jnp.float32),
            pltpu.VMEM((STEPS + 1,) + tracer.shape, jnp.float32),
            pltpu.VMEM((STEPS, width, depth, lanes), jnp.float32),
            dma((6,)),
            dma((STEPS, chunks)),
            dma((STEPS, chunks)),
            dma((STEPS, 2, chunks)),
            dma((STEPS, 2, chunks)),
            dma((STEPS, 2)),
            dma((STEPS, 2)),
            dma((STEPS + 1, 2)),
            dma((STEPS + 1, 2)),
            dma((STEPS + 1, 2, chunks, 2)),
            dma((STEPS + 1, 2, chunks, 2)),
        ],
        compiler_params=pltpu.CompilerParams(
            collective_id=0, has_side_effects=True, vmem_limit_bytes=50 * 1024 * 1024
        ),
    )(tracer, flow_y, flow_x, flow_z)


KEEP = 0


def detours(mesh):
    spots = [getattr(device, "coords", None) for device in mesh.devices[:, 0, 0]]
    if any(spot is None for spot in spots):
        return ()
    gap = lambda a, b: [i for i, (p, q) in enumerate(zip(spots[a], spots[b])) if p != q]
    found, busy = [], set()
    for a in range(len(spots)):
        for d, b in ((0, a - 1), (1, a + 1)):
            if not 0 <= b < len(spots) or len(gap(a, b)) != 2:
                continue
            kept, other = gap(a, b)[KEEP], gap(a, b)[1 - KEEP]
            for r in range(len(spots)):
                if r not in busy and gap(a, r) == [other] and gap(r, b) == [kept]:
                    busy.add(r)
                    found.append((a, d, r))
                    break
    return tuple(found)


def solution(mesh):
    counts = tuple(mesh.shape[name] for name in ("py", "px", "pz"))
    placed = P("py", "px", "pz", None)
    return jax.shard_map(
        functools.partial(local, counts, detours(mesh)),
        mesh=mesh,
        in_specs=(placed,) * 4,
        out_specs=(placed, placed),
        check_vma=False,
    )
```

```python
import functools

import jax
import jax.numpy as jnp
from jax import lax
from jax.experimental import pallas as pl
from jax.experimental.pallas import tpu as pltpu
from jax.sharding import PartitionSpec as P

STEPS = 4
MESH = pl.DeviceIdType.MESH


def divisor(size, most):
    return max(d for d in range(1, most + 1) if size % d == 0)


class Axis:
    def __init__(self, name, count):
        self.name = name
        self.me = lax.axis_index(name)
        self.to = (self.me - 1, self.me + 1)
        self.sends = (self.me > 0, self.me < count - 1)
        self.gets = (self.sends[1], self.sends[0])


def kernel(counts, relays, chunk, sub, tr, fy, fx, fz, S, E, T, F, Z, R, load, rs, rr, ys, yr, xs, xr, zs, zr, zbs, zbr):
    rows, width, depth, lanes = tr.shape
    chunks = width // chunk
    ay, ax, az = (Axis(n, c) for n, c in zip(("py", "px", "pz"), counts))
    flows = (fy, fx, fz)
    inner = rows - 2
    direct = chunks // 2

    loads = [
        pltpu.make_async_copy(tr.at[pl.ds(y, n)], T.at[0, pl.ds(1 + y, n), pl.ds(1, width)], load.at[i])
        for i, (y, n) in enumerate(((0, 1), (rows - 1, 1), (1, inner)))
    ]
    loads += [pltpu.make_async_copy(f, F.at[i], load.at[3 + i]) for i, f in enumerate(flows)]
    for copy in loads:
        copy.start()

    barrier = pltpu.get_barrier_semaphore()
    expect = 0
    for axis in (ay, ax, az):
        for d in (0, 1):
            @pl.when(axis.sends[d])
            def _():
                pl.semaphore_signal(barrier, inc=1, device_id={axis.name: axis.to[d]}, device_id_type=MESH)
            expect = expect + axis.sends[d].astype(jnp.int32)
    pairs = {frozenset((a, r)) for a, d, r in relays} | {frozenset((r, a + 2 * d - 1)) for a, d, r in relays}
    for one, other in sorted(sorted(p) for p in pairs):
        if other - one == 1:
            continue
        for a, b in ((one, other), (other, one)):
            @pl.when(ay.me == a)
            def _():
                pl.semaphore_signal(barrier, inc=1, device_id={"py": b}, device_id_type=MESH)
            expect = expect + (ay.me == a).astype(jnp.int32)

    def blank(t):
        for d in (0, 1):
            @pl.when(jnp.logical_not(ay.gets[d]))
            def _():
                @pl.loop(0, chunks)
                def _(c):
                    T[t, rows + 1 if d == 0 else 0, pl.ds(1 + c * chunk, chunk)] = jnp.zeros((chunk, depth, lanes), jnp.float32)

            @pl.when(jnp.logical_not(ax.gets[d]))
            def _():
                T[t, pl.ds(1, rows), pl.ds(width + 1 if d == 0 else 0, 1)] = jnp.zeros((rows, 1, depth, lanes), jnp.float32)

    for t in range(STEPS):
        blank(t)
    pl.semaphore_wait(barrier, expect)

    def remote(src, dst, ssem, rsem, axis, d, to=None):
        return pltpu.make_async_remote_copy(
            src_ref=src, dst_ref=dst, send_sem=ssem, recv_sem=rsem,
            device_id={axis.name: axis.to[d] if to is None else to}, device_id_type=MESH,
        )

    def ycopy(t, d, c, relay=None):
        at = c * chunk
        src = T.at[t, 1 if d == 0 else rows, pl.ds(1 + at, chunk)]
        if relay is not None:
            return remote(src, R.at[t, pl.ds(at, chunk)], ys.at[t, d, c], rr.at[t, c], ay, d, relay)
        dst = T.at[t, rows + 1 if d == 0 else 0, pl.ds(1 + at, chunk)]
        return remote(src, dst, ys.at[t, d, c], yr.at[t, d, c], ay, d)

    def detoured(t):
        return (direct, chunks) if t == 0 else (0, direct)

    def ysend(t, d, c):
        plain = ay.sends[d]
        for a, way, relay in relays:
            if way == d:
                turn = (ay.me == a) & ((c >= direct) if t == 0 else (c < direct))
                plain = plain & jnp.logical_not(turn)
                start(turn, ycopy(t, d, c, relay))
        start(plain, ycopy(t, d, c))

    def passed(t, a, d, c):
        at = c * chunk
        dst = T.at[t, rows + 1 if d == 0 else 0, pl.ds(1 + at, chunk)]
        return remote(R.at[t, pl.ds(at, chunk)], dst, rs.at[t, c], yr.at[t, d, c], ay, d, a + 2 * d - 1)

    def pass_on(t):
        for a, d, relay in relays:
            @pl.when(ay.me == relay)
            def _():
                @pl.loop(*detoured(t))
                def _(c):
                    ycopy(t, d, c, relay).wait_recv()
                    passed(t, a, d, c).start()

    def xcopy(t, d):
        src = T.at[t, pl.ds(1, rows), pl.ds(1 if d == 0 else width, 1)]
        dst = T.at[t, pl.ds(1, rows), pl.ds(width + 1 if d == 0 else 0, 1)]
        return remote(src, dst, xs.at[t, d], xr.at[t, d], ax, d)

    def zrefs(t, d, y, ny, x, nx):
        row = pl.ds(0 if d == 0 else depth - 1, 1)
        if t < STEPS:
            src = T.at[t, pl.ds(1 + y, ny), pl.ds(1 + x, nx), row]
        else:
            src = S.at[pl.ds(y, ny), pl.ds(x, nx), row]
        return src, Z.at[t, pl.ds(y, ny), pl.ds(x, nx), row]

    def zcopy(t, d):
        return remote(*zrefs(t, d, 1, inner, 0, width), zs.at[t, d], zr.at[t, d], az, d)

    def zbcopy(t, d, c, b):
        return remote(
            *zrefs(t, d, 0 if b == 0 else rows - 1, 1, c * chunk, chunk),
            zbs.at[t, d, c, b], zbr.at[t, d, c, b], az, d,
        )

    def start(flag, copy):
        @pl.when(flag)
        def _():
            copy.start()

    def arrived(flag, copy):
        @pl.when(flag)
        def _():
            copy.wait_recv()

    level = lax.broadcasted_iota(jnp.int32, (sub, depth, lanes), 1)
    known = (level == jnp.where(az.gets[0], 0, -1)) | (level == jnp.where(az.gets[1], depth - 1, -1))
    first, last = level == 0, level == depth - 1
    share = 1.0 / (depth * counts[2])

    def cells(t, y, x):
        line = T[t, 1 + y, pl.ds(x, sub + 2)]
        here, x_low, x_high = line[1:-1], line[:-2], line[2:]
        y_low = T[t, y, pl.ds(1 + x, sub)]
        y_high = T[t, y + 2, pl.ds(1 + x, sub)]
        beside = jnp.where(known, Z[t, y, pl.ds(x, sub)], 0.0)
        z_low = pltpu.roll(jnp.where(last, beside, here), 1, 1)
        z_high = pltpu.roll(jnp.where(first, beside, here), depth - 1, 1)
        spread = y_low + y_high + x_low + x_high + z_low + z_high - 6.0 * here
        new = (
            here - F[0, y, pl.ds(x, sub)] * (y_high - y_low) - F[1, y, pl.ds(x, sub)] * (x_high - x_low)
            - F[2, y, pl.ds(x, sub)] * (z_high - z_low) + 0.05 * spread
        )
        if t < STEPS - 1:
            T[t + 1, 1 + y, pl.ds(1 + x, sub)] = new
        else:
            E[y, pl.ds(x, sub)] = new
            total, reach = new, 1
            while reach < depth:
                total = total + jnp.where(level >= reach, pltpu.roll(total, reach, 1), 0.0)
                reach *= 2
            S[y, pl.ds(x, sub)] = total * share

    def add_below(y, x):
        low = Z[STEPS, y, pl.ds(x, sub), pl.ds(depth - 1, 1)]
        S[y, pl.ds(x, sub)] = S[y, pl.ds(x, sub)] + low

    def finish(c):
        for b, y in ((0, 0), (1, rows - 1)):
            zbcopy(STEPS, 1, c, b).wait_recv()

            @pl.loop(0, chunk // sub)
            def _(i):
                add_below(y, c * chunk + i * sub)
            start(az.sends[1], zbcopy(STEPS, 1, c, b))

    loads[0].wait()
    loads[1].wait()

    @pl.loop(0, chunks)
    def _(c):
        for d in (0, 1):
            ysend(0, d, c)
    loads[2].wait()
    for d in (0, 1):
        start(ax.sends[d], xcopy(0, d))
    for d in (0, 1):
        start(az.sends[d], zcopy(0, d))

        @pl.loop(0, chunks)
        def _(c):
            for b in (0, 1):
                start(az.sends[d], zbcopy(0, d, c, b))
    pass_on(0)
    for copy in loads[3:]:
        copy.wait()

    subs = width // sub
    for t in range(STEPS):
        for d in (0, 1):
            arrived(ax.gets[d], xcopy(t, d))
            arrived(az.gets[d], zcopy(t, d))

        @pl.loop(0, inner * subs)
        def _(i):
            cells(t, 1 + i // subs, (i % subs) * sub)

        if t < STEPS - 1:
            for d in (0, 1):
                start(az.sends[d], zcopy(t + 1, d))
        else:
            @pl.when(az.gets[1])
            def _():
                zcopy(STEPS, 1).wait_recv()

                @pl.loop(0, inner * subs)
                def _(i):
                    add_below(1 + i // subs, (i % subs) * sub)
            start(az.sends[1], zcopy(STEPS, 1))
        @pl.loop(0, chunks)
        def _(c):
            if t < STEPS - 1:
                @pl.when(c == direct)
                def _():
                    pass_on(t + 1)
            for d in (0, 1):
                arrived(ay.gets[d], ycopy(t, d, c))
                for b in (0, 1):
                    arrived(az.gets[d], zbcopy(t, d, c, b))
            for b, y in ((0, 0), (1, rows - 1)):
                @pl.loop(0, chunk // sub)
                def _(i):
                    cells(t, y, c * chunk + i * sub)
                if t < STEPS - 1:
                    ysend(t + 1, b, c)
                    for d in (0, 1):
                        start(az.sends[d], zbcopy(t + 1, d, c, b))
                else:
                    start(az.sends[1] & jnp.logical_not(az.gets[1]), zbcopy(STEPS, 1, c, b))
            if t == STEPS - 1:
                @pl.when(az.gets[1] & (c > 0))
                def _():
                    finish(c - 1)

        if t < STEPS - 1:
            for d in (0, 1):
                start(ax.sends[d], xcopy(t + 1, d))

    @pl.when(az.gets[1])
    def _():
        finish(chunks - 1)

    def left(flag, copy):
        @pl.when(flag)
        def _():
            copy.wait_send()

    for a, d, relay in relays:
        @pl.when(ay.me == relay)
        def _():
            for t in range(STEPS):
                @pl.loop(*detoured(t))
                def _(c):
                    passed(t, a, d, c).wait_send()

    for t in range(STEPS + 1):
        for d in (0, 1):
            if t < STEPS:
                left(ax.sends[d], xcopy(t, d))
            if t < STEPS or d == 1:
                left(az.sends[d], zcopy(t, d))

        @pl.loop(0, chunks)
        def _(c):
            for d in (0, 1):
                if t < STEPS:
                    left(ay.sends[d], ycopy(t, d, c))
                if t < STEPS or d == 1:
                    for b in (0, 1):
                        left(az.sends[d], zbcopy(t, d, c, b))


def local(counts, relays, tracer, flow_y, flow_x, flow_z):
    rows, width, depth, lanes = tracer.shape
    chunk = divisor(width, 48)
    sub = divisor(chunk, 12)
    chunks = width // chunk
    block = pltpu.VMEM(tracer.shape, jnp.float32)
    dma = pltpu.SemaphoreType.DMA
    return pl.pallas_call(
        functools.partial(kernel, counts, relays, chunk, sub),
        out_shape=(block, block),
        in_specs=[pl.BlockSpec(memory_space=pl.ANY)] * 4,
        out_specs=[pl.BlockSpec(memory_space=pltpu.VMEM)] * 2,
        scratch_shapes=[
            pltpu.VMEM((STEPS, rows + 2, width + 2, depth, lanes), jnp.float32),
            pltpu.VMEM((3,) + tracer.shape, jnp.float32),
            pltpu.VMEM((STEPS + 1,) + tracer.shape, jnp.float32),
            pltpu.VMEM((STEPS, width, depth, lanes), jnp.float32),
            dma((6,)),
            dma((STEPS, chunks)),
            dma((STEPS, chunks)),
            dma((STEPS, 2, chunks)),
            dma((STEPS, 2, chunks)),
            dma((STEPS, 2)),
            dma((STEPS, 2)),
            dma((STEPS + 1, 2)),
            dma((STEPS + 1, 2)),
            dma((STEPS + 1, 2, chunks, 2)),
            dma((STEPS + 1, 2, chunks, 2)),
        ],
        compiler_params=pltpu.CompilerParams(
            collective_id=0, has_side_effects=True, vmem_limit_bytes=50 * 1024 * 1024
        ),
    )(tracer, flow_y, flow_x, flow_z)


KEEP = 0


def detours(mesh):
    spots = [getattr(device, "coords", None) for device in mesh.devices[:, 0, 0]]
    if any(spot is None for spot in spots):
        return ()
    gap = lambda a, b: [i for i, (p, q) in enumerate(zip(spots[a], spots[b])) if p != q]
    found, busy = [], set()
    for a in range(len(spots)):
        for d, b in ((0, a - 1), (1, a + 1)):
            if not 0 <= b < len(spots) or len(gap(a, b)) != 2:
                continue
            kept, other = gap(a, b)[KEEP], gap(a, b)[1 - KEEP]
            for r in range(len(spots)):
                if r not in busy and gap(a, r) == [other] and gap(r, b) == [kept]:
                    busy.add(r)
                    found.append((a, d, r))
                    break
    return tuple(found)


def solution(mesh):
    counts = tuple(mesh.shape[name] for name in ("py", "px", "pz"))
    placed = P("py", "px", "pz", None)
    return jax.shard_map(
        functools.partial(local, counts, detours(mesh)),
        mesh=mesh,
        in_specs=(placed,) * 4,
        out_specs=(placed, placed),
        check_vma=False,
    )
```
